32 devices in a mesh: expert: 4 (over x, core), shard: 8 (over z, y).
Axes of the slice: x: 2, y: 2, z: 4, core: 2. Of those that a mesh axis runs over, the one named last changes fastest.
Arguments:
- master_gate: float32 [64, 2048, 1024], P('expert', 'shard'), may hold values from -0.1875 to 0.1875
- second_gate: bfloat16 [64, 2048, 1024], P('expert', 'shard'), may hold values from -0.0625 to 0.0625
- master_up: float32 [64, 2048, 1024], P('expert', 'shard'), may hold values from -0.1875 to 0.1875
- second_up: bfloat16 [64, 2048, 1024], P('expert', 'shard'), may hold values from -0.0625 to 0.0625
- master_down: float32 [64, 1024, 2048], P('expert', None, 'shard'), may hold values from -0.25 to 0.25
- second_down: bfloat16 [64, 1024, 2048], P('expert', None, 'shard'), may hold values from -0.09375 to 0.09375
- router_weight: float32 [2048, 64], P('shard', 'expert'), may hold values from -0.125 to 0.125
- router_gain: float32 [2048], P('shard'), may hold values from 0.25 to 1.75
Outputs:
- final_gate: bfloat16 [64, 2048, 1024], P('expert', None, 'shard')
- final_up: bfloat16 [64, 2048, 1024], P('expert', None, 'shard')
- final_down: bfloat16 [64, 1024, 2048], P('expert', 'shard')
- scale_gate: float32 [64, 1024], P('expert', 'shard')
- scale_up: float32 [64, 1024], P('expert', 'shard')
- scale_down: float32 [64, 1024], P('expert', 'shard')
- serve_router: bfloat16 [2048, 64], replicated
The draws below stay inside these ranges and needn't reach their ends.
All inputs are finite; a program needn't handle non-finite values. Where the reference program divides by a largest or mean magnitude, that divisor is 1e-20 or more.
Results may differ from the reference program's by a relative error of at most 0.001.
Values may be sent and summed in bfloat16 or wider, within the bound.
A program may use at most 192 MiB of HBM per device.

```python
import jax
import jax.numpy as jnp

EXPERTS = 64
D_MODEL = 2048
D_EXPERT = 1024


def raised(result, key, source, target, parts, factor):
    owner, partner = [(jnp.arange(result.shape[position]) // (result.shape[position] // parts)).reshape([-1 if axis == position else 1 for axis in range(result.ndim)]) for position in (source, target)]
    chosen = jax.random.permutation(key, parts)[partner]
    strong = (owner == chosen) | (owner == (partner + parts // 2) % parts)
    return jnp.where(strong, factor * result, result)


def shard_levels(rng, shape, split, low, largest):
    factor_of, own = 1.0, jax.random.fold_in(rng, 6)
    for position, blocks in split:
        heights = jnp.exp(jax.random.uniform(jax.random.fold_in(own, position), (blocks,), jnp.float32, low / len(split), largest / len(split)))
        factor_of = factor_of * jnp.repeat(heights, shape[position] // blocks).reshape([-1 if axis == position else 1 for axis in range(len(shape))])
    return factor_of


def normal_values(rng, dims, scale, bound, cuts=(), held_as=jnp.bfloat16):
    gain = shard_levels(rng, dims, cuts, -0.22, 0.18) if cuts else 1.0
    entries = jax.random.normal(rng, dims, jnp.float32) * scale * gain
    return jnp.minimum(jnp.maximum(entries, -bound), bound).astype(held_as)


def gaussian_with(key, dims, width, bound, cuts, heavy, dtype=jnp.bfloat16):
    values = width * jax.random.normal(key, dims, jnp.float32)
    if cuts:
        values = values * shard_levels(key, dims, cuts, -0.22, 0.18)
    return jnp.clip(raised(values, jax.random.fold_in(key, 3), *heavy), -bound, bound).astype(dtype)


def setup_inputs(seed: int = 0) -> dict:
    keys = jax.random.split(jax.random.key(seed), 9)
    master_gate = gaussian_with(keys[0], (EXPERTS, D_MODEL, D_EXPERT), D_MODEL ** -0.5, 0.1875, ((0, 4), (1, 8)), (1, 2, 8, 2.0), jnp.float32)
    second_gate = normal_values(keys[1], (EXPERTS, D_MODEL, D_EXPERT), (D_MODEL * 4) ** -0.5, 0.0625, ((0, 4), (1, 8)))
    master_up = gaussian_with(keys[2], (EXPERTS, D_MODEL, D_EXPERT), D_MODEL ** -0.5, 0.1875, ((0, 4), (1, 8)), (1, 2, 8, 2.0), jnp.float32)
    second_up = normal_values(keys[3], (EXPERTS, D_MODEL, D_EXPERT), (D_MODEL * 4) ** -0.5, 0.0625, ((0, 4), (1, 8)))
    master_down = gaussian_with(keys[4], (EXPERTS, D_EXPERT, D_MODEL), D_EXPERT ** -0.5, 0.25, ((0, 4), (2, 8)), (2, 1, 8, 2.0), jnp.float32)
    second_down = normal_values(keys[5], (EXPERTS, D_EXPERT, D_MODEL), (D_EXPERT * 4) ** -0.5, 0.09375, ((0, 4), (2, 8)))
    router_weight = normal_values(keys[6], (D_MODEL, EXPERTS), D_MODEL ** -0.5, 0.125, ((0, 8), (1, 4)), jnp.float32)
    router_gain = jnp.clip(1.0 + 0.15 * jax.random.normal(keys[7], (D_MODEL,), jnp.float32), 0.25, 1.75)
    return {"master_gate": master_gate, "second_gate": second_gate, "master_up": master_up, "second_up": second_up, "master_down": master_down, "second_down": second_down, "router_weight": router_weight, "router_gain": router_gain}


def reference(master_gate, second_gate, master_up, second_up, master_down, second_down, router_weight, router_gain):
    merged_gate = master_gate + second_gate.astype(jnp.float32)
    merged_up = master_up + second_up.astype(jnp.float32)
    merged_down = master_down + second_down.astype(jnp.float32)
    scale_gate = jnp.max(jnp.abs(merged_gate), axis=1)
    final_gate = (merged_gate / jnp.expand_dims(scale_gate, 1)).astype(jnp.bfloat16)
    scale_up = jnp.max(jnp.abs(merged_up), axis=1)
    final_up = (merged_up / jnp.expand_dims(scale_up, 1)).astype(jnp.bfloat16)
    scale_down = jnp.max(jnp.abs(merged_down), axis=2)
    final_down = (merged_down / jnp.expand_dims(scale_down, 2)).astype(jnp.bfloat16)
    serve_router = (router_weight * router_gain[:, None]).astype(jnp.bfloat16)
    return final_gate, final_up, final_down, scale_gate, scale_up, scale_down, serve_router
```

```python
import functools

import jax
import jax.numpy as jnp
from jax import lax
from jax.experimental import pallas as pl
from jax.experimental.pallas import tpu as pltpu
from jax.sharding import PartitionSpec as P

AHEAD = 2
LAG_REDUCE = 4
LAG_SCALE = 4
LAG = LAG_REDUCE + LAG_SCALE
HELD = AHEAD + LAG + 1
QUEUED = 4
LANES = 128


def local_wait(ref, sem):
    pltpu.make_async_copy(ref, ref, sem).wait()


def kernel(
    shards,
    groups,
    mg,
    sg,
    mu,
    su,
    md,
    sd,
    router,
    out_g,
    out_u,
    out_d,
    scale_g,
    scale_u,
    scale_d,
    out_r,
    wide,
    wide_add,
    wide_out,
    tall,
    tall_add,
    tall_out,
    part_max,
    all_max,
    scales,
    load_sem,
    add_sem,
    max_send,
    max_recv,
    scale_send,
    scale_recv,
    data_send,
    own_sem,
    data_recv,
    router_sem,
):
    experts, rows, cols = mg.shape
    piece = cols // shards
    chunks = 3 * experts
    me = lax.axis_index("shard")
    group = lax.axis_index("expert")
    others = [lax.rem(me + k, shards) for k in range(1, shards)]

    def remote(src, dst, send, recv, to):
        return pltpu.make_async_remote_copy(
            src_ref=src,
            dst_ref=dst,
            send_sem=send,
            recv_sem=recv,
            device_id=to,
            device_id_type=pl.DeviceIdType.MESH,
        )

    def between(c, body):
        pl.when(jnp.logical_and(c >= 0, c < chunks))(body)

    def loads(c):
        t, e = lax.div(c, experts), lax.rem(c, experts)
        held, near = lax.rem(c, HELD), lax.rem(c, AHEAD + 1)
        for k, (m, s, buf, add) in enumerate(
            ((mg, sg, wide, wide_add), (mu, su, wide, wide_add), (md, sd, tall, tall_add))
        ):

            @pl.when(t == k)
            def _():
                pltpu.make_async_copy(m.at[e], buf.at[held], load_sem.at[near]).start()
                pltpu.make_async_copy(s.at[e], add.at[near], add_sem.at[near]).start()

    def merge(c):
        t = lax.div(c, experts)
        held, near = lax.rem(c, HELD), lax.rem(c, AHEAD + 1)

        @pl.when(t < 2)
        def _():
            local_wait(wide.at[held], load_sem.at[near])
            local_wait(wide_add.at[near], add_sem.at[near])
            step = 32

            def body(r, best):
                at = pl.ds(pl.multiple_of(r * step, step), step)
                x = wide[held, at, :] + wide_add[near, at, :].astype(jnp.float32)
                wide[held, at, :] = x
                return jnp.maximum(best, jnp.max(jnp.abs(x).reshape(step // 8, 8, cols), axis=0))

            best = lax.fori_loop(0, rows // step, body, jnp.zeros((8, cols), jnp.float32))
            best = jnp.max(best, axis=0, keepdims=True)
            for d in range(shards):
                part_max[c, d, :, :piece] = best[:, d * piece : (d + 1) * piece]

        @pl.when(t == 2)
        def _():
            local_wait(tall.at[held], load_sem.at[near])
            local_wait(tall_add.at[near], add_sem.at[near])

            def body(d, carry):
                at = pl.ds(pl.multiple_of(d * piece, piece), piece)
                x = tall[held, at, :] + tall_add[near, at, :].astype(jnp.float32)
                tall[held, at, :] = x
                x = jnp.abs(x)
                best = x[:, :LANES]
                for k in range(1, rows // LANES):
                    best = jnp.maximum(best, x[:, k * LANES : (k + 1) * LANES])
                part_max[c, d, :, :piece] = jnp.max(best.T, axis=0, keepdims=True)
                return carry

            lax.fori_loop(0, shards, body, 0)

        all_max[c, me] = part_max[c, me]

    def send_max(c):
        for d in others:
            remote(
                part_max.at[c, d], all_max.at[c, me], max_send, max_recv.at[c], {"shard": d}
            ).start()

    def reduce(c):
        t, e = lax.div(c, experts), lax.rem(c, experts)
        local_wait(all_max.at[c, pl.ds(0, shards - 1)], max_recv.at[c])
        best = jnp.max(all_max[c], axis=0)
        scales[c, me] = best
        for k, ref in enumerate((scale_g, scale_u, scale_d)):

            @pl.when(t == k)
            def _():
                ref[pl.ds(e, 1), :] = best[:, :piece]

    def send_scale(c):
        for d in others:
            remote(
                scales.at[c, me], scales.at[c, me], scale_send, scale_recv.at[c], {"shard": d}
            ).start()

    def narrow(c):
        t = lax.div(c, experts)
        held, queued = lax.rem(c, HELD), lax.rem(c, QUEUED)
        local_wait(scales.at[c, pl.ds(0, shards - 1)], scale_recv.at[c])

        @pl.when(t < 2)
        def _():
            for d in range(shards):
                inverse = 1.0 / scales[c, d, :, :piece]
                x = wide[held, :, d * piece : (d + 1) * piece]
                wide_out[queued, d] = (x * inverse).astype(jnp.bfloat16)

        @pl.when(t == 2)
        def _():
            def body(d, carry):
                at = pl.ds(pl.multiple_of(d * piece, piece), piece)
                inverse = 1.0 / scales[c, d, :, :piece]
                inverse = jnp.broadcast_to(inverse, (LANES, piece)).T
                for k in range(rows // LANES):
                    lanes = slice(k * LANES, (k + 1) * LANES)
                    tall_out[queued, d, :, lanes] = (tall[held, at, lanes] * inverse).astype(
                        jnp.bfloat16
                    )
                return carry

            lax.fori_loop(0, shards, body, 0)

    mine = pl.ds(pl.multiple_of(me * rows, rows), rows)

    def send_data(c):
        t, e = lax.div(c, experts), lax.rem(c, experts)
        queued = lax.rem(c, QUEUED)
        for k, (src, dst) in enumerate(
            (
                (wide_out, out_g.at[e, mine, :]),
                (wide_out, out_u.at[e, mine, :]),
                (tall_out, out_d.at[e, :, mine]),
            )
        ):

            @pl.when(t == k)
            def _():
                for d in others:
                    remote(
                        src.at[queued, d],
                        dst,
                        data_send.at[queued],
                        data_recv.at[k],
                        {"shard": d},
                    ).start()
                pltpu.make_async_copy(src.at[queued, me], dst, own_sem.at[queued]).start()

    def sent_data(c):
        t = lax.div(c, experts)
        queued = lax.rem(c, QUEUED)
        for kind, src in ((t < 2, wide_out), (t == 2, tall_out)):

            @pl.when(kind)
            def _():
                local_wait(src.at[queued, pl.ds(0, shards - 1)], data_send.at[queued])
                local_wait(src.at[queued, 0], own_sem.at[queued])

    wide_r = router.shape[0]
    my_experts = pl.ds(pl.multiple_of(group * wide_r, wide_r), wide_r)

    def router_rows():
        at = out_r.at[my_experts, mine]
        for d in others:
            remote(router, at, router_sem.at[0], router_sem.at[1], {"shard": d}).start()
        pltpu.make_async_copy(router, at, router_sem.at[2]).start()

    def router_columns():
        local_wait(router, router_sem.at[2])
        gathered = out_r.at[my_experts, pl.ds(0, rows * (shards - 1))]
        local_wait(gathered, router_sem.at[1])
        for k in range(1, groups):
            to = lax.rem(group + k, groups)
            remote(
                out_r.at[my_experts],
                out_r.at[my_experts],
                router_sem.at[3],
                router_sem.at[4],
                {"expert": to},
            ).start()

    def step(i, carry):
        between(i + AHEAD, lambda: loads(i + AHEAD))
        between(i - LAG_REDUCE, lambda: reduce(i - LAG_REDUCE))
        between(i, lambda: merge(i))
        between(i - LAG_REDUCE, lambda: send_scale(i - LAG_REDUCE))
        between(i, lambda: send_max(i))
        between(i - LAG - 1, lambda: send_data(i - LAG - 1))
        pl.when(i == chunks // 2)(router_rows)
        pl.when(i == chunks)(router_columns)
        between(i - LAG - QUEUED, lambda: sent_data(i - LAG - QUEUED))
        between(i - LAG, lambda: narrow(i - LAG))
        return carry

    for c in range(AHEAD):
        loads(jnp.int32(c))
    lax.fori_loop(0, chunks + LAG + QUEUED, step, 0)

    for k, out in enumerate((out_g, out_u)):
        local_wait(out.at[:, pl.ds(0, rows * (shards - 1)), :], data_recv.at[k])
    local_wait(out_d.at[:, :, pl.ds(0, rows * (shards - 1))], data_recv.at[2])
    local_wait(part_max.at[:, pl.ds(0, shards - 1)], max_send)
    local_wait(scales.at[:, pl.ds(0, shards - 1)], scale_send)
    local_wait(out_r.at[my_experts, pl.ds(0, rows * (shards - 1))], router_sem.at[0])
    if groups > 1:
        rest = out_r.at[pl.ds(0, wide_r * (groups - 1))]
        local_wait(rest, router_sem.at[3])
        local_wait(rest, router_sem.at[4])


def by_collectives(
    master_gate,
    second_gate,
    master_up,
    second_up,
    master_down,
    second_down,
    router_weight,
    router_gain,
):
    merged_gate = master_gate + second_gate.astype(jnp.float32)
    merged_up = master_up + second_up.astype(jnp.float32)
    merged_down = master_down + second_down.astype(jnp.float32)
    scale_gate, scale_up, scale_down = lax.pmax(
        (
            jnp.max(jnp.abs(merged_gate), axis=1),
            jnp.max(jnp.abs(merged_up), axis=1),
            jnp.max(jnp.abs(merged_down), axis=2),
        ),
        "shard",
    )
    narrow_gate, narrow_up, narrow_down = (
        (merged_gate / jnp.expand_dims(scale_gate, 1)).astype(jnp.bfloat16),
        (merged_up / jnp.expand_dims(scale_up, 1)).astype(jnp.bfloat16),
        (merged_down / jnp.expand_dims(scale_down, 2)).astype(jnp.bfloat16),
    )
    final_gate, final_up = (
        lax.all_to_all(narrow_gate, "shard", split_axis=2, concat_axis=1, tiled=True),
        lax.all_to_all(narrow_up, "shard", split_axis=2, concat_axis=1, tiled=True),
    )
    final_down = lax.all_to_all(narrow_down, "shard", split_axis=1, concat_axis=2, tiled=True)
    scale_gate = lax.dynamic_slice_in_dim(
        scale_gate, lax.axis_index("shard") * final_gate.shape[2], final_gate.shape[2], axis=1
    )
    scale_up = lax.dynamic_slice_in_dim(
        scale_up, lax.axis_index("shard") * final_up.shape[2], final_up.shape[2], axis=1
    )
    scale_down = lax.dynamic_slice_in_dim(
        scale_down, lax.axis_index("shard") * final_down.shape[1], final_down.shape[1], axis=1
    )
    part_router = (router_weight * router_gain[:, None]).astype(jnp.bfloat16)
    row_router = lax.all_gather(part_router, "shard", axis=0, tiled=True)
    serve_router = lax.all_gather(row_router, "expert", axis=1, tiled=True)
    return (final_gate, final_up, final_down, scale_gate, scale_up, scale_down, serve_router)


def per_device(
    shards,
    groups,
    master_gate,
    second_gate,
    master_up,
    second_up,
    master_down,
    second_down,
    router_weight,
    router_gain,
):
    experts, rows, cols = master_gate.shape
    piece = cols // shards
    chunks = 3 * experts
    if piece % LANES or rows % LANES:
        return by_collectives(
            master_gate,
            second_gate,
            master_up,
            second_up,
            master_down,
            second_down,
            router_weight,
            router_gain,
        )
    router = (router_weight * router_gain[:, None]).astype(jnp.bfloat16).T
    anywhere = pl.BlockSpec(memory_space=pl.ANY)
    vmem = pl.BlockSpec(memory_space=pltpu.VMEM)
    f32, bf16, dma = jnp.float32, jnp.bfloat16, pltpu.SemaphoreType.DMA
    shape = jax.ShapeDtypeStruct
    small = max(piece, LANES)
    *outs, served = pl.pallas_call(
        functools.partial(kernel, shards, groups),
        out_shape=(
            shape((experts, rows * shards, piece), bf16),
            shape((experts, rows * shards, piece), bf16),
            shape((experts, piece, rows * shards), bf16),
            shape((experts, piece), f32),
            shape((experts, piece), f32),
            shape((experts, piece), f32),
            shape((router.shape[0] * groups, rows * shards), bf16),
        ),
        in_specs=[anywhere] * 6 + [vmem],
        out_specs=(anywhere, anywhere, anywhere, vmem, vmem, vmem, anywhere),
        scratch_shapes=[
            pltpu.VMEM((HELD, rows, cols), f32),
            pltpu.VMEM((AHEAD + 1, rows, cols), bf16),
            pltpu.VMEM((QUEUED, shards, rows, piece), bf16),
            pltpu.VMEM((HELD, cols, rows), f32),
            pltpu.VMEM((AHEAD + 1, cols, rows), bf16),
            pltpu.VMEM((QUEUED, shards, piece, rows), bf16),
            pltpu.VMEM((chunks, shards, 1, small), f32),
            pltpu.VMEM((chunks, shards, 1, small), f32),
            pltpu.VMEM((chunks, shards, 1, small), f32),
            dma((AHEAD + 1,)),
            dma((AHEAD + 1,)),
            dma,
            dma((chunks,)),
            dma,
            dma((chunks,)),
            dma((QUEUED,)),
            dma((QUEUED,)),
            dma((3,)),
            dma((5,)),
        ],
        compiler_params=pltpu.CompilerParams(
            has_side_effects=True, vmem_limit_bytes=60 * 1024 * 1024
        ),
    )(master_gate, second_gate, master_up, second_up, master_down, second_down, router)
    return (*outs, served.T)


def solution(mesh):
    in_specs = (
        P("expert", "shard", None),
        P("expert", "shard", None),
        P("expert", "shard", None),
        P("expert", "shard", None),
        P("expert", None, "shard"),
        P("expert", None, "shard"),
        P("shard", "expert"),
        P("shard"),
    )
    out_specs = (
        P("expert", None, "shard"),
        P("expert", None, "shard"),
        P("expert", "shard", None),
        P("expert", "shard"),
        P("expert", "shard"),
        P("expert", "shard"),
        P(),
    )
    return jax.shard_map(
        functools.partial(per_device, mesh.shape["shard"], mesh.shape["expert"]),
        mesh=mesh,
        in_specs=in_specs,
        out_specs=out_specs,
        check_vma=False,
    )
```
